128 devices in a mesh: tp: 16 (over z, x_hi, core), fs: 8 (over y, x_lo).
Axes of the slice: x: 4 (x_hi: 2, x_lo: 2; x = x_hi * 2 + x_lo), y: 4, z: 4, core: 2. Of those that a mesh axis runs over, the one named last changes fastest.
Arguments:
- tokens: bfloat16 [512, 8192], P(('tp', 'fs')), may hold values from -6 to 6
- gate_weight: bfloat16 [8192, 29568], P('fs', 'tp'), may hold values from -0.0625 to 0.0625
- up_weight: bfloat16 [8192, 29568], P('fs', 'tp'), may hold values from -0.0625 to 0.0625
- down_weight: bfloat16 [29568, 8192], P('tp', 'fs'), may hold values from -0.046875 to 0.046875
Outputs:
- mixed: bfloat16 [512, 8192], P(None, ('fs', 'tp'))
The draws below stay inside these ranges and needn't reach their ends.
All inputs are finite; a program needn't handle non-finite values.
Results may differ from the reference program's by a relative error of at most 0.0049.
Values may be sent and summed in bfloat16 or wider, within the bound.
No kernel may reach another device: no remote copies, remote signals or barrier semaphores. Data moves between devices by JAX's collectives and lax.ppermute only.
A program may use at most 64 MiB of HBM per device.

```python
import jax
import jax.numpy as jnp

D = 8192
FF = 29568
TOKENS = 512


def strengthened(values, key, source, target, shards_of, factor):
    owner, partner = [(jnp.arange(values.shape[dim]) // (values.shape[dim] // shards_of)).reshape([-1 if axis == dim else 1 for axis in range(values.ndim)]) for dim in (source, target)]
    chosen = jax.random.permutation(key, shards_of)[partner]
    strong = (owner == chosen) | (owner == (partner + shards_of // 2) % shards_of)
    return jnp.where(strong, factor * values, values)


def shard_levels(own_key, shape, pieces, low, high):
    def one(dim, blocks):
        draws = jax.random.uniform(jax.random.fold_in(jax.random.fold_in(own_key, 6), dim), (blocks,), jnp.float32, low / len(pieces), high / len(pieces))
        return jnp.repeat(jnp.exp(draws), shape[dim] // blocks).reshape((-1,) + (1,) * (len(shape) - dim - 1))

    level = one(*pieces[0])
    for cut in pieces[1:]:
        level = level * one(*cut)
    return level


def bell_draw(own_key, extent, spread, bound, pieces=(), held_as=jnp.bfloat16):
    loudness = shard_levels(own_key, extent, pieces, -0.22, 0.18) if pieces else 1.0
    entries = jax.random.normal(own_key, extent, jnp.float32) * spread * loudness
    return jnp.minimum(jnp.maximum(entries, -bound), bound).astype(held_as)


def gaussian_with(own_key, shape, width, most, split, heavy, kind=jnp.bfloat16):
    array = width * jax.random.normal(own_key, shape, jnp.float32)
    if split:
        array = array * shard_levels(own_key, shape, split, -0.22, 0.18)
    return jnp.clip(strengthened(array, jax.random.fold_in(own_key, 3), *heavy), -most, most).astype(kind)


def setup_inputs(seed: int = 0) -> dict:
    key_list = jax.random.split(jax.random.key(seed), 5)
    tokens = bell_draw(key_list[0], (TOKENS, D), 1.0, 6.0, ((0, 128),))
    gate_weight = bell_draw(key_list[1], (D, FF), D ** -0.5, 0.0625, ((0, 8), (1, 16)))
    up_weight = bell_draw(key_list[2], (D, FF), D ** -0.5, 0.0625, ((0, 8), (1, 16)))
    down_weight = gaussian_with(key_list[3], (FF, D), FF ** -0.5, 0.046875, ((0, 16), (1, 8)), (0, 1, 16, 2.0))
    return dict(tokens=tokens, gate_weight=gate_weight, up_weight=up_weight, down_weight=down_weight)


def reference(tokens, gate_weight, up_weight, down_weight):
    gate = jnp.dot(tokens, gate_weight, preferred_element_type=jnp.float32)
    up = jnp.dot(tokens, up_weight, preferred_element_type=jnp.float32)
    hidden = (jax.nn.silu(gate) * up).astype(jnp.bfloat16)
    mixed = jnp.dot(hidden, down_weight, preferred_element_type=jnp.float32)
    return mixed.astype(jnp.bfloat16)
```

```python
import jax
import jax.numpy as jnp
from jax import lax
from jax.sharding import Mesh
from jax.sharding import PartitionSpec as P

FS = ("y", "xl")
TP = ("z", "xh", "c")
TP_FS = TP + FS
FS_TP = FS + TP
ROWS = 232


def exchanged(pieces, axes):
    return lax.all_to_all(pieces, axes, split_axis=0, concat_axis=0, tiled=True)


def gathered(shard, axes, count):
    copies = jnp.broadcast_to(shard, (count, *shard.shape))
    return exchanged(copies, axes).reshape(-1, *shard.shape[1:])


def units_by_device(part):
    padded = jnp.pad(part.astype(jnp.bfloat16), ((0, 8 * ROWS - part.shape[0]), (0, 0)))
    return padded.reshape(8, ROWS, -1)


def body(tokens, gate_weight, up_weight, down_weight):
    by_feature = lax.all_to_all(tokens, FS, split_axis=1, concat_axis=0, tiled=True)
    rows = gathered(by_feature, TP, 16)
    units = gate_weight.shape[1]
    contract = (((0,), (1,)), ((), ()))
    gate_part = lax.dot_general(gate_weight, rows, contract, preferred_element_type=jnp.float32)
    up_part = lax.dot_general(up_weight, rows, contract, preferred_element_type=jnp.float32)
    parts = jnp.concatenate([units_by_device(gate_part), units_by_device(up_part)], axis=1)
    sums = exchanged(parts, FS).astype(jnp.float32).sum(axis=0)
    gate, up = sums[:ROWS], sums[ROWS:]
    hidden = (jax.nn.silu(gate) * up).astype(jnp.bfloat16)
    group_hidden = gathered(hidden, FS, 8)[:units]
    contract = (((0,), (0,)), ((), ()))
    partial_cols = lax.dot_general(down_weight, group_hidden, contract, preferred_element_type=jnp.float32)
    arrived = exchanged(partial_cols.astype(jnp.bfloat16).reshape(16, 64, -1), TP)
    return arrived.astype(jnp.float32).sum(axis=0).astype(jnp.bfloat16).T


def solution(mesh):
    finer = Mesh(mesh.devices.reshape(4, 2, 2, 4, 2), TP_FS)
    in_specs = (P(TP_FS, None), P(FS, TP), P(FS, TP), P(TP, FS))
    out_specs = P(None, FS_TP)
    return jax.shard_map(body, mesh=finer, in_specs=in_specs, out_specs=out_specs, check_vma=False)
```

```python
import functools

import jax
import jax.numpy as jnp
from jax import lax
from jax.experimental import pallas as pl
from jax.experimental.pallas import tpu as pltpu
from jax.sharding import Mesh
from jax.sharding import PartitionSpec as P

FS = ("y", "xl")
TP = ("z", "xh", "c")
TP_FS = TP + FS
FS_TP = FS + TP
FIRST, SECOND = 112, 120
SPLIT = 8 * FIRST
TURNS = (2, 1, 3)
f32, bf16 = jnp.float32, jnp.bfloat16


def at(array, index):
    return lax.dynamic_index_in_dim(array, index, 0, keepdims=False)


def put(buffer, piece, index):
    return lax.dynamic_update_index_in_dim(buffer, piece, index, 0)


def swapped(piece, axis):
    return lax.ppermute(piece, axis, [(0, 1), (1, 0)])


def turned(piece, axis, step):
    return lax.ppermute(piece, axis, [(i, (i + step) % 4) for i in range(4)])


def pair_of(own, other, place):
    both = jnp.zeros((2, *own.shape), own.dtype)
    return put(put(both, own, place), other, 1 - place)


def gathered(own, axis, place):
    pieces = put(jnp.zeros((4, *own.shape), own.dtype), own, place)
    for step in TURNS:
        pieces = put(pieces, turned(own, axis, step), (place - step) % 4)
    return pieces


def activated(sums):
    return (jax.nn.silu(sums[..., 0, :, :]) * sums[..., 1, :, :]).astype(bf16)


def products_kernel(height, where, rows, gate, up, out, held, sems):
    steps, span = held.shape[0], out.shape[2]
    pieces = height // span
    copies = []
    for step in range(steps):
        for kind, weight in enumerate((gate, up)):
            window = weight.at[pl.ds(pl.multiple_of(where[step], 8), height)]
            copies.append(pltpu.make_async_copy(window, held.at[step, kind], sems.at[step, kind]))
            copies[-1].start()
    for step in range(steps):
        for kind in range(2):
            copies[2 * step + kind].wait()
            result = lax.dot_general(held[step, kind], rows[...], (((1,), (1,)), ((), ())), preferred_element_type=f32)
            for piece in range(pieces):
                out[step * pieces + piece, kind] = result[piece * span : (piece + 1) * span].astype(out.dtype)


def products(rows, gate, up, starts, pieces, span, dtype):
    height, (count, depth) = pieces * span, rows.shape
    steps = len(starts)
    vmem, hbm = (pl.BlockSpec(memory_space=space) for space in (pltpu.VMEM, pltpu.HBM))
    flops = 4 * steps * height * count * depth
    return pl.pallas_call(
        functools.partial(products_kernel, height),
        out_shape=jax.ShapeDtypeStruct((steps * pieces, 2, span, count), dtype),
        in_specs=[pl.BlockSpec(memory_space=pltpu.SMEM), vmem, hbm, hbm],
        out_specs=vmem,
        scratch_shapes=[pltpu.VMEM((steps, 2, height, depth), bf16), pltpu.SemaphoreType.DMA((steps, 2))],
        compiler_params=pltpu.CompilerParams(vmem_limit_bytes=14 << 20),
        cost_estimate=pl.CostEstimate(flops=flops, bytes_accessed=4 * steps * height * depth, transcendentals=0),
    )(jnp.stack(starts).astype(jnp.int32), rows, gate, up)


def down_kernel(where, weight, group, own, out):
    core = where[0]
    half = weight.shape[1] // 2
    for part in range(2):
        block = weight[:, part * half : (part + 1) * half]
        result = lax.dot_general(block, group[...], (((0,), (0,)), ((), ())), preferred_element_type=f32)
        for i in range(4):
            low, high = result[128 * i : 128 * i + 64], result[128 * i + 64 : 128 * (i + 1)]
            own[4 * part + i] = jnp.where(core == 0, low, high)
            out[4 * part + i] = jnp.where(core == 0, high, low)


def down_products(weight, group, core):
    (units, columns), count = weight.shape, group.shape[1]
    vmem = pl.BlockSpec(memory_space=pltpu.VMEM)
    shape = jax.ShapeDtypeStruct((8, columns // 16, count), f32)
    return pl.pallas_call(
        down_kernel,
        out_shape=(shape, shape),
        in_specs=[pl.BlockSpec(memory_space=pltpu.SMEM), vmem, vmem],
        out_specs=(vmem, vmem),
        compiler_params=pltpu.CompilerParams(vmem_limit_bytes=20 << 20),
        cost_estimate=pl.CostEstimate(flops=2 * units * columns * count, bytes_accessed=2 * units * columns, transcendentals=0),
        name="down",
    )(jnp.reshape(core, (1,)).astype(jnp.int32), weight, group)


def body(tokens, gate_weight, up_weight, down_weight):
    z, xh, c, y, xl = (lax.axis_index(name) for name in TP_FS)
    units = gate_weight.shape[1]
    gate, up = (pltpu.with_memory_space_constraint(w.T, pltpu.HBM) for w in (gate_weight, up_weight))

    by_feature = lax.all_to_all(tokens, FS, split_axis=1, concat_axis=0, tiled=True)
    line = pair_of(by_feature, swapped(by_feature, "xh"), xh)
    plane = gathered(line, "z", z).reshape(8, 1, *by_feature.shape)
    rows = jnp.zeros((8, 2, *by_feature.shape), bf16)
    rows = lax.dynamic_update_slice(rows, plane, (0, c, 0, 0))
    rows = lax.dynamic_update_slice(rows, swapped(plane, "c"), (0, 1 - c, 0, 0))
    rows = rows.reshape(512, -1)

    def second_starts(half):
        start = SPLIT + half * (units - SPLIT - 4 * SECOND)
        return [start, start + 2 * SECOND]

    def first_start(turn):
        return (y + turn) % 4 * (2 * FIRST)

    q_out = products(rows, gate, up, second_starts(1 - xl), 2, SECOND, bf16)
    q_got = swapped(q_out, "xl")
    p_out = products(rows, gate, up, [first_start(turn) for turn in TURNS], 2, FIRST, bf16)
    p_got = [turned(p_out[2 * i : 2 * i + 2], "y", turn) for i, turn in enumerate(TURNS)]
    q_own = products(rows, gate, up, second_starts(xl), 2, SECOND, f32)
    p_own = products(rows, gate, up, [first_start(0)], 2, FIRST, f32)

    def q_sum(turn):
        place = (y + turn) % 4
        return at(q_own, place) + at(q_got, place).astype(f32)

    def q_send(turn):
        return q_sum(turn).astype(bf16)

    q_arrived = [turned(q_send(turn), "y", turn).astype(f32) for turn in TURNS]
    p_sum = p_own + sum(piece.astype(f32) for piece in p_got)
    p_arrived = swapped(at(p_sum, 1 - xl).astype(bf16), "xl").astype(f32)
    p_hidden = activated(at(p_sum, xl) + p_arrived)
    q_hidden = activated(q_sum(0) + sum(q_arrived))

    def placed(group, piece, row):
        return lax.dynamic_update_slice(group, piece, (row, 0))

    def p_row(y_at, xl_at):
        return (y_at * 2 + xl_at) * FIRST

    def q_row(y_at, xl_at):
        return SPLIT + xl_at * (units - SPLIT - 4 * SECOND) + y_at * SECOND

    p_column = gathered(p_hidden, "y", y)
    q_other = swapped(q_hidden, "xl")
    q_pair = jnp.stack([q_hidden, q_other])
    group = placed(jnp.zeros((units, 512), bf16), q_hidden, q_row(y, xl))
    group = placed(group, q_other, q_row(y, 1 - xl))
    p_other = swapped(p_column, "xl")
    for place in range(4):
        group = placed(group, p_column[place], p_row(place, xl))
        group = placed(group, p_other[place], p_row(place, 1 - xl))
    for turn in TURNS:
        arrived, place = turned(q_pair, "y", turn), (y - turn) % 4
        group = placed(group, arrived[0], q_row(place, xl))
        group = placed(group, arrived[1], q_row(place, 1 - xl))

    own_part, out_part = down_products(down_weight, group, c)
    sums = (own_part + swapped(out_part, "c")).reshape(4, 2, 64, -1)
    z_sum = at(sums, z)
    for turn in TURNS:
        z_sum += turned(at(sums, (z + turn) % 4).astype(bf16), "z", turn).astype(f32)
    total = at(z_sum, xh) + swapped(at(z_sum, 1 - xh).astype(bf16), "xh").astype(f32)
    return total.astype(bf16).T


def solution(mesh):
    finer = Mesh(mesh.devices.reshape(4, 2, 2, 4, 2), TP_FS)
    in_specs = (P(TP_FS, None), P(FS, TP), P(FS, TP), P(TP, FS))
    out_specs = P(None, FS_TP)
    return jax.shard_map(body, mesh=finer, in_specs=in_specs, out_specs=out_specs, check_vma=False)
```
